32 devices in a mesh: group: 2 (over y), station: 4 (over z), tm: 2 (over x), chan: 2 (over core).
Axes of the slice: x: 2, y: 2, z: 4, core: 2. Of those that a mesh axis runs over, the one named last changes fastest.
Arguments:
- voltages: bfloat16 [8, 128, 2, 96, 256], P(('group', 'station'), 'chan', None, None, 'tm'), parts along dimension 0, may hold values from -6 to 6
- delays: int32 [8], P(('group', 'station')), parts along dimension 0, may hold values from 0 to 16, as said below
- tap_sets: int32 [8, 128], P(('group', 'station'), 'chan'), parts along dimension 0, may hold values from 0 to 15
- tap_table: bfloat16 [16, 16], replicated, may hold values from -1.5 to 1.5
- weights: bfloat16 [8, 128, 2, 96, 128], P(('group', 'station'), 'chan'), parts along dimension 0, may hold values from -0.3125 to 0.3125
Outputs:
- array_beams: bfloat16 [256, 2, 128, 256], P(('group', 'chan', 'station'), None, None, 'tm'), parts along dimension 0
The draws below stay inside these ranges and needn't reach their ends.
There are 2 independent parts, one for each index of `group`. The reference program is written for one: setup_inputs(seed, part) draws one part's arguments, and reference() takes and returns one part's arrays. A program takes and returns all parts, laid end to end along the dimension named above; an argument that names none is the same for every part. Nothing has to cross between parts.
Inputs may be any that keep to these rules, and one draw needn't show every extreme that they name: `delays`: every delay lies in 0 to 16, and some station has delay 16.
All inputs are finite; a program needn't handle non-finite values.
Results may differ from the reference program's by a relative error of at most 0.0049.
Values may be sent and summed in bfloat16 or wider, within the bound.
A program may use at most 64 MiB of HBM per device.

```python
import jax
import jax.numpy as jnp
from jax import lax

ANTENNA_COUNT = 96
BEAM_TOTAL = 128
TAPS = 16
MAXD = 16
NSETS = 16
STATION_TOTAL = 4
FREQUENCY_BINS = 128
TIME_SAMPLES = 256


def draw_delays(key, part):
    drawn = jax.random.randint(key, (STATION_TOTAL,), 0, MAXD + 1)
    chosen = jax.random.randint(jax.random.fold_in(key, 7), (), 0, STATION_TOTAL)
    positions = jnp.arange(STATION_TOTAL)
    return jnp.where(positions == chosen, MAXD, drawn).astype(jnp.int32)


def plant(array, own_key, least, largest):
    longest = array.shape.index(max(array.shape))
    spots = []
    for shift in (0, 1):
        where = [jax.random.randint(jax.random.fold_in(own_key, axis), (), 0, length) for axis, length in enumerate(array.shape)]
        where[longest] = (where[longest] + shift) % array.shape[longest]
        spots.append(tuple(where))
    return array.at[spots[0]].set(least).at[spots[1]].set(largest)


def raised(values, key, source, target, shards_of, factor):
    def block_of(axis_at):
        return (jnp.arange(values.shape[axis_at]) // (values.shape[axis_at] // shards_of)).reshape((-1,) + (1,) * (values.ndim - 1 - axis_at))

    near = jax.random.permutation(key, shards_of)[block_of(target)]
    other_side = (block_of(target) + shards_of // 2) % shards_of
    return jnp.where((block_of(source) == near) | (block_of(source) == other_side), factor * values, values)


def levels(key, dims, cuts, low, top_value):
    def one(dim, parts):
        heights = jax.random.uniform(jax.random.fold_in(jax.random.fold_in(key, 6), dim), (parts,), jnp.float32, low / len(cuts), top_value / len(cuts))
        return jnp.repeat(jnp.exp(heights), dims[dim] // parts).reshape((-1,) + (1,) * (len(dims) - dim - 1))

    level = one(*cuts[0])
    for cut in cuts[1:]:
        level = level * one(*cut)
    return level


def gaussian(own_key, dims, width, reach, pieces=(), dtype=jnp.bfloat16):
    loudness = levels(own_key, dims, pieces, -0.22, 0.18) if pieces else 1.0
    array = jax.random.normal(own_key, dims, jnp.float32) * width * loudness
    return jnp.minimum(jnp.maximum(array, -reach), reach).astype(dtype)


def bell_draw_with(key, shape, spread, reach, split, heavy, held_as=jnp.bfloat16):
    values = spread * jax.random.normal(key, shape, jnp.float32)
    if split:
        values = values * levels(key, shape, split, -0.22, 0.18)
    return jnp.clip(raised(values, jax.random.fold_in(key, 3), *heavy), -reach, reach).astype(held_as)


def setup_inputs(seed: int = 0, part: int = 0) -> dict:
    key_of = jax.random.split(jax.random.key(seed), 6)
    part_splits = jax.random.split(jax.random.fold_in(key_of[5], part), 6)
    voltages = gaussian(part_splits[0], (STATION_TOTAL, FREQUENCY_BINS, 2, ANTENNA_COUNT, TIME_SAMPLES), 1.0, 6.0, ((0, 4), (1, 2), (4, 2)))
    delays = draw_delays(jax.random.fold_in(jax.random.fold_in(key_of[5], part), 71), part)
    tap_sets = plant(jax.random.randint(part_splits[2], (STATION_TOTAL, FREQUENCY_BINS), 0, NSETS), jax.random.fold_in(part_splits[2], 1), 0, NSETS - 1).astype(jnp.int32)
    tap_table = gaussian(key_of[3], (NSETS, TAPS), 0.25, 1.5)
    weights = bell_draw_with(part_splits[4], (STATION_TOTAL, FREQUENCY_BINS, 2, ANTENNA_COUNT, BEAM_TOTAL), (2 * ANTENNA_COUNT * STATION_TOTAL) ** -0.5, 0.3125, ((0, 4), (1, 2)), (0, 1, 4, 2.0))
    return {"voltages": voltages, "delays": delays, "tap_sets": tap_sets, "tap_table": tap_table, "weights": weights}


def reference(voltages, delays, tap_sets, tap_table, weights):
    halo_len = MAXD + TAPS - 1
    table_f32 = tap_table.astype(jnp.float32)

    def one_station(running, station_item):
        samples, delay_now, chosen_sets, steer = station_item
        samples_f32 = samples.astype(jnp.float32)
        padded = jnp.pad(samples_f32, ((0, 0), (0, 0), (0, 0), (halo_len, 0)))
        coefficients = table_f32[chosen_sets]
        summed_taps = jnp.zeros(samples_f32.shape, jnp.float32)
        for tap_index in range(TAPS):
            begin = (halo_len - delay_now - tap_index).astype(jnp.int32)
            shifted = lax.dynamic_slice_in_dim(padded, begin, TIME_SAMPLES, 3)
            summed_taps = summed_taps + coefficients[:, tap_index][:, None, None, None] * shifted
        delayed_voltages = lax.optimization_barrier(summed_taps.astype(jnp.bfloat16)).astype(jnp.float32)
        steer_f32 = steer.astype(jnp.float32)
        real_in = delayed_voltages[:, 0]
        imag_in = delayed_voltages[:, 1]
        real_part = jnp.einsum('cat,cab->cbt', real_in, steer_f32[:, 0]) - jnp.einsum('cat,cab->cbt', imag_in, steer_f32[:, 1])
        imag_part = jnp.einsum('cat,cab->cbt', real_in, steer_f32[:, 1]) + jnp.einsum('cat,cab->cbt', imag_in, steer_f32[:, 0])
        return running + jnp.stack([real_part, imag_part], axis=1), None

    start_sum = jnp.zeros((FREQUENCY_BINS, 2, BEAM_TOTAL, TIME_SAMPLES), jnp.float32)
    result, unused = lax.scan(one_station, start_sum, (voltages, delays, tap_sets, weights))
    return result.astype(jnp.bfloat16)
```

```python
import functools

import jax
import jax.numpy as jnp
from jax import lax
from jax.experimental import pallas as pl
from jax.experimental.pallas import tpu as pltpu
from jax.sharding import PartitionSpec as P

MAXD = 16
MESH = pl.DeviceIdType.MESH
CHUNK = 2


def kernel(
    n, tm_count, sizes, tap_sets, delays, taps, v_hbm, w_hbm, out_buf,
    v_buf, w_buf, band, halo_out, halo_in, acc_out, acc_in,
    v_sem, w_sem, hs_sem, hr_sem, as_sem, ar_sem,
):
    channels, parts, antennas, beams, time_len, chunk, pad = sizes
    rows = channels // n
    half = rows // 2
    per_half = half // chunk
    rows_in = parts * antennas
    folds = time_len // pad
    fold_rows = rows_in // folds
    set_count, tap_count = taps.shape
    items = n * per_half

    me = lax.axis_index("station")
    tm = lax.axis_index("tm")
    right, left = lax.rem(me + 1, n), lax.rem(me + n - 1, n)
    later, earlier = lax.rem(tm + 1, tm_count), lax.rem(tm + tm_count - 1, tm_count)

    def place(it, side):
        step, k = it // per_half, lax.rem(it, per_half)
        odd = lax.rem(step, 2)
        offset = n // 2 - odd - step // 2
        if side == 0:
            block, second = lax.rem(me + offset, n), odd
        else:
            block, second = lax.rem(me + n - offset, n), 1 - odd
        within = second * half + k * chunk
        return block * rows + within, within

    def v_copy(it, side):
        first, _ = place(it, side)
        span = pl.ds(first, chunk)
        return pltpu.make_async_copy(v_hbm.at[span], v_buf.at[span], v_sem.at[it, side])

    def w_copy(it, side):
        first, _ = place(it, side)
        span = pl.ds(first, chunk)
        return pltpu.make_async_copy(w_hbm.at[span], w_buf.at[span], w_sem.at[it, side])

    def halo_copy(it, side):
        return pltpu.make_async_remote_copy(
            src_ref=halo_out.at[it, side],
            dst_ref=halo_in.at[it, side],
            send_sem=hs_sem.at[it, side],
            recv_sem=hr_sem.at[it, side],
            device_id={"tm": later},
            device_id_type=MESH,
        )

    def sum_copy(it, side):
        return pltpu.make_async_remote_copy(
            src_ref=acc_out.at[it, side],
            dst_ref=acc_in.at[it, side],
            send_sem=as_sem.at[it, side],
            recv_sem=ar_sem.at[it, side],
            device_id={"station": right if side == 0 else left},
            device_id_type=MESH,
        )

    def start_loads(it, carry):
        for side in (0, 1):
            v_copy(it, side).start()
            w_copy(it, side).start()
        return carry

    lax.fori_loop(0, items, start_loads, 0)

    barrier = pltpu.get_barrier_semaphore()
    for target in ({"station": left}, {"station": right}, {"tm": earlier}, {"tm": later}):
        pl.semaphore_signal(barrier, inc=1, device_id=target, device_id_type=MESH)

    from_row = lax.broadcasted_iota(jnp.int32, (folds * time_len, time_len), 0)
    to_lane = lax.broadcasted_iota(jnp.int32, (folds * time_len, time_len), 1)
    wanted = (to_lane // pad) * time_len + lax.rem(to_lane, pad) + time_len - pad
    picker = (from_row == wanted).astype(jnp.float32).astype(jnp.bfloat16)

    def pack(it, side):
        first, _ = place(it, side)
        v_copy(it, side).wait()
        for c in range(chunk):
            wide = jnp.concatenate(
                [v_buf[first + c, pl.ds(q * fold_rows, fold_rows), :] for q in range(folds)], axis=1
            )
            halo_out[it, side, c] = jnp.dot(
                wide, picker, preferred_element_type=jnp.float32
            ).astype(jnp.bfloat16)
        halo_copy(it, side).start()

    pl.semaphore_wait(barrier, 4)

    def pack_first(it, carry):
        pack(it, 0)
        pack(it, 1)
        return carry

    lead = per_half
    lax.fori_loop(0, lead, pack_first, 0)

    out_pos = lax.broadcasted_iota(jnp.int32, (time_len, 2 * time_len), 0)
    column = lax.broadcasted_iota(jnp.int32, (time_len, 2 * time_len), 1)
    in_pos = jnp.where(column < time_len, column, lax.rem(column, pad) - pad)
    usable = (column < time_len) | (tm > 0)
    lag = jnp.where(usable, out_pos - delays[0] - in_pos, -1)

    def make_band(m, carry):
        values = jnp.zeros((time_len, 2 * time_len), jnp.float32)
        for k in range(tap_count):
            values = jnp.where(lag == k, taps[m, k], values)
        band[m] = values.astype(jnp.bfloat16)
        return carry

    lax.fori_loop(0, set_count, make_band, 0)

    fold_lane = lax.broadcasted_iota(jnp.int32, (fold_rows, time_len), 1) // pad

    def beams_of(it, side, c):
        first, _ = place(it, side)
        channel = first + c
        rim = halo_in[it, side, c]
        rims = jnp.concatenate(
            [jnp.where(fold_lane == q, rim, jnp.zeros_like(rim)) for q in range(folds)], axis=0
        )
        window = jnp.concatenate([v_buf[channel], rims], axis=1)
        filt = band[tap_sets[0, channel]]
        delayed = lax.dot_general(
            filt, window, (((1,), (1,)), ((), ())), preferred_element_type=jnp.float32
        ).astype(jnp.bfloat16)
        wr = w_buf[channel, pl.ds(0, antennas), :]
        wi = w_buf[channel, pl.ds(antennas, antennas), :]
        steer = jnp.concatenate(
            [jnp.concatenate([wr, wi], axis=1), jnp.concatenate([-wi, wr], axis=1)], axis=0
        )
        return jnp.dot(delayed, steer, preferred_element_type=jnp.float32)

    def ready(it, side):
        halo_copy(it, side).wait_recv()
        w_copy(it, side).wait()

    def head(it, carry):
        for side in (0, 1):
            pack(it + lead, side)
        for side in (0, 1):
            ready(it, side)
            for c in range(chunk):
                acc_out[it, side, c] = beams_of(it, side, c).astype(jnp.bfloat16)
            sum_copy(it, side).start()
        return carry

    lax.fori_loop(0, 2 * per_half, head, 0)

    def middle(it, carry):
        for side in (0, 1):
            pack(it + lead, side)
        for side in (0, 1):
            ready(it, side)
            before = it - 2 * per_half
            sum_copy(before, side).wait_recv()
            for c in range(chunk):
                total = beams_of(it, side, c) + acc_in[before, side, c].astype(jnp.float32)
                acc_out[it, side, c] = total.astype(jnp.bfloat16)
            sum_copy(it, side).start()
        return carry

    lax.fori_loop(2 * per_half, items - per_half, middle, 0)

    def last(it, carry):
        for side in (0, 1):
            ready(it, side)
            _, within = place(it, side)
            same, other = it - 2 * per_half, it - per_half
            sums = [beams_of(it, side, c) for c in range(chunk)]
            sum_copy(same, side).wait_recv()
            sum_copy(other, 1 - side).wait_recv()
            for c in range(chunk):
                total = sums[c] + acc_in[same, side, c].astype(jnp.float32)
                total = total + acc_in[other, 1 - side, c].astype(jnp.float32)
                out_buf[within + c] = total.T.astype(jnp.bfloat16)
        return carry

    lax.fori_loop(items - per_half, items, last, 0)

    def drain_halo(it, carry):
        for side in (0, 1):
            halo_copy(it, side).wait_send()
        return carry

    lax.fori_loop(0, items, drain_halo, 0)

    def drain_sums(it, carry):
        for side in (0, 1):
            sum_copy(it, side).wait_send()
        return carry

    lax.fori_loop(0, items - per_half, drain_sums, 0)


def body(voltages, delays, tap_sets, tap_table, weights):
    _, channels, parts, antennas, time_len = voltages.shape
    beams = weights.shape[-1]
    set_count, tap_count = tap_table.shape
    n = lax.axis_size("station")
    tm_count = lax.axis_size("tm")
    rows = channels // n
    chunk = min(CHUNK, rows // 2)
    per_half = rows // 2 // chunk
    items = n * per_half
    pad = MAXD + tap_count
    rows_in = parts * antennas
    fold_rows = rows_in * pad // time_len
    sizes = (channels, parts, antennas, beams, time_len, chunk, pad)
    sent = items - per_half
    bf16 = jnp.bfloat16
    dma = pltpu.SemaphoreType.DMA
    smem = pl.BlockSpec(memory_space=pltpu.SMEM)
    in_hbm = pl.BlockSpec(memory_space=pltpu.HBM)
    result = pl.pallas_call(
        functools.partial(kernel, n, tm_count, sizes),
        out_shape=jax.ShapeDtypeStruct((rows, 2 * beams, time_len), bf16),
        in_specs=[smem, smem, smem, in_hbm, in_hbm],
        out_specs=pl.BlockSpec(memory_space=pltpu.VMEM),
        scratch_shapes=[
            pltpu.VMEM((channels, rows_in, time_len), bf16),
            pltpu.VMEM((channels, rows_in, beams), bf16),
            pltpu.VMEM((set_count, time_len, 2 * time_len), bf16),
            pltpu.VMEM((items, 2, chunk, fold_rows, time_len), bf16),
            pltpu.VMEM((items, 2, chunk, fold_rows, time_len), bf16),
            pltpu.VMEM((sent, 2, chunk, time_len, 2 * beams), bf16),
            pltpu.VMEM((sent, 2, chunk, time_len, 2 * beams), bf16),
            dma((items, 2)),
            dma((items, 2)),
            dma((items, 2)),
            dma((items, 2)),
            dma((sent, 2)),
            dma((sent, 2)),
        ],
        compiler_params=pltpu.CompilerParams(
            collective_id=0, has_side_effects=True, vmem_limit_bytes=48 * 1024 * 1024
        ),
    )(
        tap_sets,
        delays,
        tap_table.astype(jnp.float32),
        voltages.reshape(channels, rows_in, time_len),
        weights.reshape(channels, rows_in, beams),
    )
    return result.reshape(rows, 2, beams, time_len)


def solution(mesh):
    return jax.shard_map(
        body,
        mesh=mesh,
        in_specs=(
            P(("group", "station"), "chan", None, None, "tm"),
            P(("group", "station")),
            P(("group", "station"), "chan"),
            P(),
            P(("group", "station"), "chan", None, None, None),
        ),
        out_specs=P(("group", "chan", "station"), None, None, "tm"),
        check_vma=False,
    )
```

```python
import functools

import jax
import jax.numpy as jnp
from jax import lax
from jax.experimental import pallas as pl
from jax.experimental.pallas import tpu as pltpu
from jax.sharding import PartitionSpec as P

MAXD = 16
MESH = pl.DeviceIdType.MESH
CHUNK = 8
LEAD = 2


def kernel(
    n, tm_count, sizes, tap_sets, delays, taps, v_hbm, w_hbm, out_buf,
    v_buf, w_buf, band, tap_values, halo_out, halo_in, own_sum, acc_out, acc_in,
    v_sem, w_sem, hs_sem, hr_sem, as_sem, ar_sem,
):
    channels, parts, antennas, beams, time_len, chunk, pad = sizes
    rows = channels // n
    per_block = rows // chunk
    rows_in = parts * antennas
    folds = time_len // pad
    fold_rows = rows_in // folds
    set_count, tap_count = taps.shape
    sends = (n - 1) * per_block
    items = n * per_block

    me = lax.axis_index("station")
    tm = lax.axis_index("tm")
    right, left = lax.rem(me + 1, n), lax.rem(me + n - 1, n)
    later, earlier = lax.rem(tm + 1, tm_count), lax.rem(tm + tm_count - 1, tm_count)

    def place(it, side):
        step, k = it // per_block, lax.rem(it, per_block)
        own = step // (n - 1)
        if side == 0:
            block = (1 - own) * (n - 1 - step) + own * me
            valid = (n - 1 - step > me) | (step == n - 1)
        else:
            block, valid = step, step < me
        return block * per_block + k, valid

    def v_copy(at):
        span = pl.ds(at * chunk, chunk)
        return pltpu.make_async_copy(v_hbm.at[span], v_buf.at[span], v_sem.at[at])

    def w_copy(at):
        span = pl.ds(at * chunk, chunk)
        return pltpu.make_async_copy(w_hbm.at[span], w_buf.at[span], w_sem.at[at])

    def halo_copy(at):
        return pltpu.make_async_remote_copy(
            src_ref=halo_out.at[at],
            dst_ref=halo_in.at[at],
            send_sem=hs_sem.at[at],
            recv_sem=hr_sem.at[at],
            device_id={"tm": later},
            device_id_type=MESH,
        )

    def sum_copy(it, side):
        return pltpu.make_async_remote_copy(
            src_ref=acc_out.at[it, side],
            dst_ref=acc_in.at[it, side],
            send_sem=as_sem.at[it, side],
            recv_sem=ar_sem.at[it, side],
            device_id={"station": right if side == 0 else left},
            device_id_type=MESH,
        )

    def each(start, stop, act):
        def one(it, carry):
            for side in (0, 1):
                at, valid = place(it, side)

                @pl.when(valid)
                def _(at=at, side=side):
                    act(it, side, at)

            return carry

        lax.fori_loop(start, stop, one, 0)

    def start_loads(it, side, at):
        v_copy(at).start()
        w_copy(at).start()

    each(0, items, start_loads)

    barrier = pltpu.get_barrier_semaphore()
    for target in ({"station": left}, {"station": right}, {"tm": earlier}, {"tm": later}):
        pl.semaphore_signal(barrier, inc=1, device_id=target, device_id_type=MESH)

    from_row = lax.broadcasted_iota(jnp.int32, (folds * time_len, time_len), 0)
    to_lane = lax.broadcasted_iota(jnp.int32, (folds * time_len, time_len), 1)
    wanted = (to_lane // pad) * time_len + lax.rem(to_lane, pad) + time_len - pad
    picker = (from_row == wanted).astype(jnp.float32).astype(jnp.bfloat16)

    def pack(it, side, at):
        v_copy(at).wait()
        for c in range(chunk):
            wide = jnp.concatenate(
                [v_buf[at * chunk + c, pl.ds(q * fold_rows, fold_rows), :] for q in range(folds)], axis=1
            )
            halo_out[at, c] = jnp.dot(
                wide, picker, preferred_element_type=jnp.float32
            ).astype(jnp.bfloat16)
        halo_copy(at).start()

    pl.semaphore_wait(barrier, 4)

    lead = min(LEAD, per_block)
    each(0, lead, pack)

    out_pos = lax.broadcasted_iota(jnp.int32, (time_len, 2 * time_len), 0)
    column = lax.broadcasted_iota(jnp.int32, (time_len, 2 * time_len), 1)
    in_pos = jnp.where(column < time_len, column, lax.rem(column, pad) - pad)
    usable = (column < time_len) | (tm > 0)
    lag = jnp.where(usable, out_pos - delays[0] - in_pos, -1)
    tap_values[...] = taps[...].astype(jnp.float32)

    def make_band(m, carry):
        row = tap_values[pl.ds(m, 1), :]
        values = jnp.zeros((time_len, 2 * time_len), jnp.float32)
        for k in range(tap_count):
            values = jnp.where(lag == k, row[:, k : k + 1], values)
        band[m] = values.astype(jnp.bfloat16)
        return carry

    lax.fori_loop(0, set_count, make_band, 0)

    fold_lane = lax.broadcasted_iota(jnp.int32, (fold_rows, time_len), 1) // pad

    def beams_of(at, c):
        channel = at * chunk + c
        rim = halo_in[at, c]
        rims = jnp.concatenate(
            [jnp.where(fold_lane == q, rim, jnp.zeros_like(rim)) for q in range(folds)], axis=0
        )
        window = jnp.concatenate([v_buf[channel], rims], axis=1)
        filt = band[tap_sets[0, channel]]
        delayed = lax.dot_general(
            filt, window, (((1,), (1,)), ((), ())), preferred_element_type=jnp.float32
        ).astype(jnp.bfloat16)
        wr = w_buf[channel, pl.ds(0, antennas), :]
        wi = w_buf[channel, pl.ds(antennas, antennas), :]
        steer = jnp.concatenate(
            [jnp.concatenate([wr, wi], axis=1), jnp.concatenate([-wi, wr], axis=1)], axis=0
        )
        return jnp.dot(delayed, steer, preferred_element_type=jnp.float32)

    def compute(at):
        halo_copy(at).wait_recv()
        w_copy(at).wait()
        for c in range(chunk):
            own_sum[c] = beams_of(at, c)

    def send(it, side, at):
        compute(at)
        first = me == (0 if side == 0 else n - 1)

        @pl.when(first)
        def _():
            for c in range(chunk):
                acc_out[it, side, c] = own_sum[c].astype(jnp.bfloat16)

        @pl.when(jnp.logical_not(first))
        def _():
            sum_copy(it, side).wait_recv()
            for c in range(chunk):
                total = own_sum[c] + acc_in[it, side, c].astype(jnp.float32)
                acc_out[it, side, c] = total.astype(jnp.bfloat16)

        sum_copy(it, side).start()

    def send_step(it, carry):
        each(it + lead, it + lead + 1, pack)
        each(it, it + 1, send)
        return carry

    lax.fori_loop(0, sends, send_step, 0)

    def last(k, carry):
        at = me * per_block + k

        @pl.when(k + lead < per_block)
        def _():
            pack(0, 0, at + lead)

        compute(at)

        @pl.when(me < n - 1)
        def _():
            slot = me * per_block + k
            sum_copy(slot, 1).wait_recv()
            for c in range(chunk):
                own_sum[c] += acc_in[slot, 1, c].astype(jnp.float32)

        @pl.when(me > 0)
        def _():
            slot = (n - 1 - me) * per_block + k
            sum_copy(slot, 0).wait_recv()
            for c in range(chunk):
                own_sum[c] += acc_in[slot, 0, c].astype(jnp.float32)

        for c in range(chunk):
            out_buf[k * chunk + c] = own_sum[c].T.astype(jnp.bfloat16)
        return carry

    lax.fori_loop(0, per_block, last, 0)

    each(0, items, lambda it, side, at: halo_copy(at).wait_send())
    each(0, sends, lambda it, side, at: sum_copy(it, side).wait_send())


def body(voltages, delays, tap_sets, tap_table, weights):
    _, channels, parts, antennas, time_len = voltages.shape
    beams = weights.shape[-1]
    set_count, tap_count = tap_table.shape
    n = lax.axis_size("station")
    tm_count = lax.axis_size("tm")
    rows = channels // n
    chunk = min(CHUNK, rows)
    items = channels // chunk
    pad = MAXD + tap_count
    rows_in = parts * antennas
    fold_rows = rows_in * pad // time_len
    sizes = (channels, parts, antennas, beams, time_len, chunk, pad)
    sent = items - rows // chunk
    bf16 = jnp.bfloat16
    dma = pltpu.SemaphoreType.DMA
    smem = pl.BlockSpec(memory_space=pltpu.SMEM)
    in_hbm = pl.BlockSpec(memory_space=pltpu.HBM)
    result = pl.pallas_call(
        functools.partial(kernel, n, tm_count, sizes),
        out_shape=jax.ShapeDtypeStruct((rows, 2 * beams, time_len), bf16),
        in_specs=[smem, smem, pl.BlockSpec(memory_space=pltpu.VMEM), in_hbm, in_hbm],
        out_specs=pl.BlockSpec(memory_space=pltpu.VMEM),
        scratch_shapes=[
            pltpu.VMEM((channels, rows_in, time_len), bf16),
            pltpu.VMEM((channels, rows_in, beams), bf16),
            pltpu.VMEM((set_count, time_len, 2 * time_len), bf16),
            pltpu.VMEM((set_count, tap_count), jnp.float32),
            pltpu.VMEM((items, chunk, fold_rows, time_len), bf16),
            pltpu.VMEM((items, chunk, fold_rows, time_len), bf16),
            pltpu.VMEM((chunk, time_len, 2 * beams), jnp.float32),
            pltpu.VMEM((sent, 2, chunk, time_len, 2 * beams), bf16),
            pltpu.VMEM((sent, 2, chunk, time_len, 2 * beams), bf16),
            dma((items,)),
            dma((items,)),
            dma((items,)),
            dma((items,)),
            dma((sent, 2)),
            dma((sent, 2)),
        ],
        compiler_params=pltpu.CompilerParams(
            collective_id=0, has_side_effects=True, vmem_limit_bytes=60 * 1024 * 1024
        ),
    )(
        tap_sets,
        delays,
        tap_table,
        voltages.reshape(channels, rows_in, time_len),
        weights.reshape(channels, rows_in, beams),
    )
    return result.reshape(rows, 2, beams, time_len)


def solution(mesh):
    return jax.shard_map(
        body,
        mesh=mesh,
        in_specs=(
            P(("group", "station"), "chan", None, None, "tm"),
            P(("group", "station")),
            P(("group", "station"), "chan"),
            P(),
            P(("group", "station"), "chan", None, None, None),
        ),
        out_specs=P(("group", "chan", "station"), None, None, "tm"),
        check_vma=False,
    )
```
